8 devices in a mesh: data: 1 (over z), expert: 8 (over y, x, core).
Axes of the slice: x: 2, y: 2, z: 1, core: 2. Of those that a mesh axis runs over, the one named last changes fastest.
Arguments:
- x_a: bfloat16 [8192, 1024], P(('data', 'expert'))
- x_b: bfloat16 [8192, 1024], P(('data', 'expert'))
- dy_b: bfloat16 [8192, 1024], P(('data', 'expert'))
- eid_a: int32 [8192, 8], P(('data', 'expert'))
- slot_a: int32 [8192, 8], P(('data', 'expert'))
- gate_a: bfloat16 [8192, 8], P(('data', 'expert'))
- eid_b: int32 [8192, 8], P(('data', 'expert'))
- slot_b: int32 [8192, 8], P(('data', 'expert'))
- gate_b: bfloat16 [8192, 8], P(('data', 'expert'))
- u_b: bfloat16 [32, 4096, 1024], P(('data', 'expert'))
- norm_1: bfloat16 [1024], replicated
- norm_2: bfloat16 [1024], replicated
- w_q: bfloat16 [1024, 16, 64], replicated
- w_k: bfloat16 [1024, 8, 64], replicated
- w_v: bfloat16 [1024, 8, 64], replicated
- w_o: bfloat16 [16, 64, 1024], replicated
- w_1: bfloat16 [32, 1024, 512], P('expert')
- w_2: bfloat16 [32, 512, 1024], P('expert')
- w_3: bfloat16 [32, 1024, 512], P('expert')
Outputs:
- output 1: bfloat16 [8192, 1024], P(('data', 'expert'))
- output 2: bfloat16 [8192, 1024], P(('data', 'expert'))
- output 3: float32 [32, 1024, 512], P(('data', 'expert'))
- output 4: float32 [32, 512, 1024], P(('data', 'expert'))
- output 5: float32 [32, 1024, 512], P(('data', 'expert'))
- output 6: float32 [8, 1024, 16, 64], P(('data', 'expert'))
- output 7: float32 [8, 1024, 8, 64], P(('data', 'expert'))
- output 8: float32 [8, 1024, 8, 64], P(('data', 'expert'))
- output 9: float32 [8, 16, 64, 1024], P(('data', 'expert'))
- output 10: float32 [8, 1024], P(('data', 'expert'))
- output 11: float32 [8, 1024], P(('data', 'expert'))
All inputs are finite; a program needn't handle non-finite values.
Results may differ from the reference program's by a relative error of at most 0.018046.
Values are sent between devices in bfloat16 or wider.
A program may use at most 1 GiB of HBM per device.

```python
import jax
import jax.numpy as jnp
from jax import lax

GROUP = 8
TOKENS = 1024
MODEL_DIM = 1024
HEADS = 16
KV_HEADS = 8
HEAD_DIM = 64
EXPERTS = 32
FF_DIM = 512
TOP_K = 8
ROWS = GROUP * TOKENS
CAPACITY = ((2 * TOP_K * TOKENS + 8 * EXPERTS - 1) // (8 * EXPERTS)) * 8
HOT_ROWS = min(TOKENS, CAPACITY + CAPACITY // 4)
NORM_EPS = 1e-6


def draw_routing(route_key):
    key_score, key_hot = jax.random.split(route_key, 2)
    scores = jax.random.randint(key_score, (GROUP, TOKENS, EXPERTS), 0, 2 ** 20)
    hot_ids = jax.random.randint(key_hot, (GROUP,), 0, EXPERTS)
    boosted = (jnp.arange(TOKENS)[None, :, None] < HOT_ROWS) & (jnp.arange(EXPERTS)[None, None, :] == hot_ids[:, None, None])
    scores = (scores + boosted.astype(scores.dtype) * 2 ** 20) * EXPERTS + jnp.arange(EXPERTS)
    _, expert_ids = lax.top_k(scores, TOP_K)
    flat_ids = expert_ids.reshape(GROUP, TOKENS * TOP_K)
    onehot = (flat_ids[:, :, None] == jnp.arange(EXPERTS)[None, None, :]).astype(jnp.int32)
    arrival = jnp.sum((jnp.cumsum(onehot, axis=1) - onehot) * onehot, axis=2)
    slots = jnp.where(arrival < CAPACITY, arrival, -1)
    return expert_ids.reshape(ROWS, TOP_K).astype(jnp.int32), slots.reshape(ROWS, TOP_K).astype(jnp.int32)


def slot_columns(slots):
    device_of = jnp.arange(ROWS)[:, None] // TOKENS
    return jnp.where(slots >= 0, device_of * CAPACITY + slots, GROUP * CAPACITY)


def saved_inputs(value_key, expert_ids, slots):
    filled = jnp.zeros((EXPERTS, GROUP * CAPACITY), jnp.float32).at[expert_ids, slot_columns(slots)].set(1.0, mode='drop')
    values = jax.random.normal(value_key, (EXPERTS, GROUP * CAPACITY, MODEL_DIM), jnp.float32)
    return (values * filled[:, :, None]).astype(jnp.bfloat16)


def normal_draw(draw_key, dims, scale):
    return (jax.random.normal(draw_key, dims, jnp.float32) * scale).astype(jnp.bfloat16)


def setup_inputs(seed: int = 0, part: int = 0) -> dict:
    part_key = jax.random.fold_in(jax.random.key(seed), part)
    key_list = jax.random.split(part_key, 8)
    shared = jax.random.split(jax.random.key(seed + 1), 9)
    eid_a, slot_a = draw_routing(key_list[0])
    eid_b, slot_b = draw_routing(key_list[1])
    gate_a = (jax.random.uniform(key_list[2], (ROWS, TOP_K), jnp.float32, 0.5, 1.5) / TOP_K).astype(jnp.bfloat16)
    gate_b = (jax.random.uniform(key_list[3], (ROWS, TOP_K), jnp.float32, 0.5, 1.5) / TOP_K).astype(jnp.bfloat16)
    return {
        'x_a': normal_draw(key_list[4], (ROWS, MODEL_DIM), 1.0),
        'x_b': normal_draw(key_list[5], (ROWS, MODEL_DIM), 1.0),
        'dy_b': normal_draw(key_list[6], (ROWS, MODEL_DIM), 1.0),
        'eid_a': eid_a,
        'slot_a': slot_a,
        'gate_a': gate_a,
        'eid_b': eid_b,
        'slot_b': slot_b,
        'gate_b': gate_b,
        'u_b': saved_inputs(key_list[7], eid_b, slot_b),
        'norm_1': (1.0 + 0.3 * jax.random.normal(shared[0], (MODEL_DIM,), jnp.float32)).astype(jnp.bfloat16),
        'norm_2': (1.0 + 0.3 * jax.random.normal(shared[1], (MODEL_DIM,), jnp.float32)).astype(jnp.bfloat16),
        'w_q': normal_draw(shared[2], (MODEL_DIM, HEADS, HEAD_DIM), MODEL_DIM ** -0.5),
        'w_k': normal_draw(shared[3], (MODEL_DIM, KV_HEADS, HEAD_DIM), MODEL_DIM ** -0.5),
        'w_v': normal_draw(shared[4], (MODEL_DIM, KV_HEADS, HEAD_DIM), MODEL_DIM ** -0.5),
        'w_o': normal_draw(shared[5], (HEADS, HEAD_DIM, MODEL_DIM), 2.0 * (HEADS * HEAD_DIM) ** -0.5),
        'w_1': normal_draw(shared[6], (EXPERTS, MODEL_DIM, FF_DIM), MODEL_DIM ** -0.5),
        'w_2': normal_draw(shared[7], (EXPERTS, FF_DIM, MODEL_DIM), 3.0 * FF_DIM ** -0.5),
        'w_3': normal_draw(shared[8], (EXPERTS, MODEL_DIM, FF_DIM), MODEL_DIM ** -0.5),
    }


def rms_norm(values, gain):
    wide = values.astype(jnp.float32)
    scaled = wide * lax.rsqrt(jnp.mean(wide * wide, axis=-1, keepdims=True) + NORM_EPS)
    return (scaled * gain.astype(jnp.float32)).astype(jnp.bfloat16)


def add_rows(first, second):
    return (first.astype(jnp.float32) + second.astype(jnp.float32)).astype(jnp.bfloat16)


def attn_out(x_rows, norm_gain, w_q, w_k, w_v, w_o):
    normed = rms_norm(x_rows, norm_gain).astype(jnp.float32)
    query = jnp.einsum('td,dhe->the', normed, w_q.astype(jnp.float32)).astype(jnp.bfloat16)
    query = query.reshape(TOKENS, KV_HEADS, HEADS // KV_HEADS, HEAD_DIM).astype(jnp.float32)
    key_proj = jnp.einsum('td,dge->tge', normed, w_k.astype(jnp.float32)).astype(jnp.bfloat16).astype(jnp.float32)
    val_proj = jnp.einsum('td,dge->tge', normed, w_v.astype(jnp.float32)).astype(jnp.bfloat16).astype(jnp.float32)
    scores = jnp.einsum('tgre,mge->grtm', query, key_proj) * HEAD_DIM ** -0.5
    causal = jnp.arange(TOKENS)[:, None] >= jnp.arange(TOKENS)[None, :]
    scores = jnp.where(causal, scores, -1e30)
    probs = jax.nn.softmax(scores, axis=-1).astype(jnp.bfloat16).astype(jnp.float32)
    context = jnp.einsum('grtm,mge->tgre', probs, val_proj).astype(jnp.bfloat16)
    context = context.reshape(TOKENS, HEADS, HEAD_DIM).astype(jnp.float32)
    return jnp.einsum('the,hed->td', context, w_o.astype(jnp.float32)).astype(jnp.bfloat16)


def expert_forward(buf, w_1, w_2, w_3):
    act_1 = jnp.dot(buf, w_1, preferred_element_type=jnp.float32).astype(jnp.bfloat16).astype(jnp.float32)
    act_3 = jnp.dot(buf, w_3, preferred_element_type=jnp.float32).astype(jnp.bfloat16).astype(jnp.float32)
    hidden = (act_1 * jax.nn.sigmoid(act_1) * act_3).astype(jnp.bfloat16)
    return jnp.dot(hidden, w_2, preferred_element_type=jnp.float32).astype(jnp.bfloat16)


def expert_backward(saved, d_out, w_1, w_2, w_3):
    pre_1 = jnp.dot(saved, w_1, preferred_element_type=jnp.float32).astype(jnp.bfloat16).astype(jnp.float32)
    pre_3 = jnp.dot(saved, w_3, preferred_element_type=jnp.float32).astype(jnp.bfloat16).astype(jnp.float32)
    sigma = jax.nn.sigmoid(pre_1)
    silu_1 = pre_1 * sigma
    hidden = (silu_1 * pre_3).astype(jnp.bfloat16)
    grad_w2 = jnp.dot(hidden.T, d_out, preferred_element_type=jnp.float32)
    grad_hid = jnp.dot(d_out, w_2.T, preferred_element_type=jnp.float32).astype(jnp.bfloat16).astype(jnp.float32)
    grad_a1 = (grad_hid * pre_3 * sigma * (1.0 + pre_1 * (1.0 - sigma))).astype(jnp.bfloat16)
    grad_a3 = (grad_hid * silu_1).astype(jnp.bfloat16)
    grad_w1 = jnp.dot(saved.T, grad_a1, preferred_element_type=jnp.float32)
    grad_w3 = jnp.dot(saved.T, grad_a3, preferred_element_type=jnp.float32)
    grad_in = (jnp.dot(grad_a1, w_1.T, preferred_element_type=jnp.float32) + jnp.dot(grad_a3, w_3.T, preferred_element_type=jnp.float32)).astype(jnp.bfloat16)
    return grad_w1, grad_w2, grad_w3, grad_in


def pick_rows(buf, expert_ids, columns):
    padded = jnp.concatenate([buf, jnp.zeros((EXPERTS, 1, MODEL_DIM), buf.dtype)], axis=1)
    return padded[expert_ids, columns]


def reference(x_a, x_b, dy_b, eid_a, slot_a, gate_a, eid_b, slot_b, gate_b, u_b, norm_1, norm_2, w_q, w_k, w_v, w_o, w_1, w_2, w_3):
    def forward_rows(x_dev):
        return add_rows(x_dev, attn_out(x_dev, norm_1, w_q, w_k, w_v, w_o))
    h_a = lax.map(forward_rows, x_a.reshape(GROUP, TOKENS, MODEL_DIM)).reshape(ROWS, MODEL_DIM)
    u_a = rms_norm(h_a, norm_2)
    cols_a = slot_columns(slot_a)
    buf_a = jnp.zeros((EXPERTS, GROUP * CAPACITY, MODEL_DIM), jnp.bfloat16).at[eid_a, cols_a].set(jnp.broadcast_to(u_a[:, None, :], (ROWS, TOP_K, MODEL_DIM)), mode='drop')
    out_a = lax.map(lambda item: expert_forward(item[0], item[1], item[2], item[3]), (buf_a, w_1, w_2, w_3))
    picked = pick_rows(out_a, eid_a, cols_a).astype(jnp.float32)
    mixed = jnp.sum(gate_a.astype(jnp.float32)[:, :, None] * picked, axis=1)
    y_a = (h_a.astype(jnp.float32) + mixed).astype(jnp.bfloat16)
    cols_b = slot_columns(slot_b)
    grad_rows = (gate_b.astype(jnp.float32)[:, :, None] * dy_b.astype(jnp.float32)[:, None, :]).astype(jnp.bfloat16)
    d_out = jnp.zeros((EXPERTS, GROUP * CAPACITY, MODEL_DIM), jnp.bfloat16).at[eid_b, cols_b].set(grad_rows, mode='drop')
    grad_w1, grad_w2, grad_w3, grad_in = lax.map(lambda item: expert_backward(item[0], item[1], item[2], item[3], item[4]), (u_b, d_out, w_1, w_2, w_3))
    du_rows = jnp.sum(pick_rows(grad_in, eid_b, cols_b).astype(jnp.float32), axis=1).astype(jnp.bfloat16)
    def backward_rows(item):
        x_dev, dy_dev, du_dev = item
        attn_val, attn_pull = jax.vjp(attn_out, x_dev, norm_1, w_q, w_k, w_v, w_o)
        h_dev = add_rows(x_dev, attn_val)
        _, norm_pull = jax.vjp(rms_norm, h_dev, norm_2)
        dh_norm, grad_n2 = norm_pull(du_dev)
        dh_dev = add_rows(dy_dev, dh_norm)
        grad_x, grad_n1, grad_q, grad_k, grad_v, grad_o = attn_pull(dh_dev)
        return (add_rows(dh_dev, grad_x), grad_q.astype(jnp.float32), grad_k.astype(jnp.float32), grad_v.astype(jnp.float32), grad_o.astype(jnp.float32), grad_n1.astype(jnp.float32), grad_n2.astype(jnp.float32))
    dx_b, g_q, g_k, g_v, g_o, g_n1, g_n2 = lax.map(backward_rows, (x_b.reshape(GROUP, TOKENS, MODEL_DIM), dy_b.reshape(GROUP, TOKENS, MODEL_DIM), du_rows.reshape(GROUP, TOKENS, MODEL_DIM)))
    return (y_a, dx_b.reshape(ROWS, MODEL_DIM), grad_w1, grad_w2, grad_w3, g_q, g_k, g_v, g_o, g_n1, g_n2)
```

```python
import functools

import jax
import jax.numpy as jnp
from jax import lax
from jax.experimental import pallas as pl
from jax.experimental.pallas import tpu as pltpu
from jax.sharding import PartitionSpec as P

NORM_EPS = 1e-6


def expert_map(expert_ids, slot_ids, gates, experts):
    held = (expert_ids[None] == jnp.arange(experts)[:, None, None]) & (slot_ids >= 0)[None]
    slot_map = jnp.max(jnp.where(held, slot_ids[None], -1), axis=2).astype(jnp.float32)
    gate_map = jnp.sum(jnp.where(held, gates.astype(jnp.float32)[None], 0.0), axis=2)
    return slot_map, gate_map


VMEM_BYTES = 60 * 2 ** 20
NT = (((1,), (1,)), ((), ()))
TN = (((0,), (0,)), ((), ()))


def mm(lhs, rhs, dims=(((1,), (0,)), ((), ()))):
    return lax.dot_general(lhs, rhs, dims, preferred_element_type=jnp.float32)


def round_bf16(values):
    return values.astype(jnp.bfloat16).astype(jnp.float32)


def fill_sizes(capacity):
    return (capacity * 9 // 16 // 16 * 16, capacity)


def by_fill(count, capacity, body):
    low = 0
    for size in fill_sizes(capacity):
        pl.when((count > low) & (count <= size))(functools.partial(body, size))
        low = size


def forward_kernel(capacity, counts, slot_rows, slot_cols, gate_cols, x_ref, w1_ref, w3_ref, w2_ref, out_ref):
    source = pl.program_id(0)
    tokens = x_ref.shape[1]
    out_ref[...] = jnp.zeros_like(out_ref)
    for expert in range(w1_ref.shape[0]):
        def body(size, expert=expert):
            rows = lax.broadcasted_iota(jnp.int32, (size, tokens), 0)
            hot = jnp.where(slot_rows[0, expert:expert + 1, :] == rows, 1.0, 0.0).astype(jnp.bfloat16)
            buf = mm(hot, x_ref[0]).astype(jnp.bfloat16)
            act_1 = round_bf16(mm(buf, w1_ref[expert]))
            act_3 = round_bf16(mm(buf, w3_ref[expert]))
            hidden = (act_1 * jax.nn.sigmoid(act_1) * act_3).astype(jnp.bfloat16)
            out = mm(hidden, w2_ref[expert]).astype(jnp.bfloat16)
            cols = lax.broadcasted_iota(jnp.int32, (tokens, size), 1)
            mix = jnp.where(slot_cols[0, :, expert:expert + 1] == cols, gate_cols[0, :, expert:expert + 1], 0.0).astype(jnp.bfloat16)
            out_ref[0] += mm(mix, out)

        by_fill(counts[source, expert], capacity, body)


def experts_forward(counts, slot_rows, slot_cols, gate_cols, rows, w_1, w_3, w_2, capacity):
    group, tokens, model_dim = rows.shape
    local, _, ff = w_1.shape
    whole = lambda shape: pl.BlockSpec(shape, lambda p: (0, 0, 0), pipeline_mode=pl.Buffered(1))
    by_source = lambda shape: pl.BlockSpec(shape, lambda p: (p, 0, 0))
    return pl.pallas_call(
        functools.partial(forward_kernel, capacity),
        out_shape=jax.ShapeDtypeStruct((group, tokens, model_dim), jnp.float32),
        grid=(group,),
        in_specs=[pl.BlockSpec(memory_space=pltpu.SMEM), by_source((1, local, tokens)), by_source((1, tokens, local)), by_source((1, tokens, local)),
                  by_source((1, tokens, model_dim)), whole(w_1.shape), whole(w_3.shape), whole(w_2.shape)],
        out_specs=by_source((1, tokens, model_dim)),
        compiler_params=pltpu.CompilerParams(dimension_semantics=('arbitrary',), vmem_limit_bytes=VMEM_BYTES),
        cost_estimate=pl.CostEstimate(flops=group * local * capacity * model_dim * (4 * tokens + 6 * ff) // 2, bytes_accessed=group * tokens * model_dim * 6, transcendentals=0),
        name='experts_forward',
    )(counts, slot_rows, slot_cols, gate_cols, rows, w_1, w_3, w_2)


def backward_kernel(capacity, counts, slot_rows, gate_rows, dy_ref, u_ref, w1_ref, w3_ref, w2_ref, du_ref, g1_ref, g2_ref, g3_ref):
    expert, source = pl.program_id(0), pl.program_id(1)
    tokens = dy_ref.shape[1]

    @pl.when(source == 0)
    def _():
        g1_ref[...] = jnp.zeros_like(g1_ref)
        g2_ref[...] = jnp.zeros_like(g2_ref)
        g3_ref[...] = jnp.zeros_like(g3_ref)

    def body(size):
        rows = lax.broadcasted_iota(jnp.int32, (size, tokens), 0)
        scaled = jnp.where(slot_rows[0, 0] == rows, gate_rows[0, 0], 0.0).astype(jnp.bfloat16)
        d_out = mm(scaled, dy_ref[0]).astype(jnp.bfloat16)
        saved = u_ref[0, :size, :]
        pre_1 = round_bf16(mm(saved, w1_ref[0]))
        pre_3 = round_bf16(mm(saved, w3_ref[0]))
        sigma = jax.nn.sigmoid(pre_1)
        silu_1 = pre_1 * sigma
        hidden = (silu_1 * pre_3).astype(jnp.bfloat16)
        g2_ref[0] += mm(hidden, d_out, TN)
        grad_hid = round_bf16(mm(d_out, w2_ref[0], NT))
        grad_a1 = (grad_hid * pre_3 * sigma * (1.0 + pre_1 * (1.0 - sigma))).astype(jnp.bfloat16)
        grad_a3 = (grad_hid * silu_1).astype(jnp.bfloat16)
        g1_ref[0] += mm(saved, grad_a1, TN)
        g3_ref[0] += mm(saved, grad_a3, TN)
        du_ref[0, :size, :] = (mm(grad_a1, w1_ref[0], NT) + mm(grad_a3, w3_ref[0], NT)).astype(jnp.bfloat16)

    by_fill(counts[source, expert], capacity, body)


def experts_backward(counts, slot_rows, gate_rows, dy_rows, saved, w_1, w_3, w_2, capacity):
    group, tokens, model_dim = dy_rows.shape
    local, _, ff = w_1.shape
    by_pair = lambda shape: pl.BlockSpec(shape, lambda e, p: (p, e, 0, 0))
    by_expert = lambda shape: pl.BlockSpec(shape, lambda e, p: (e, 0, 0))
    by_slot = pl.BlockSpec((1, capacity, model_dim), lambda e, p: (e, p, 0))
    return pl.pallas_call(
        functools.partial(backward_kernel, capacity),
        out_shape=(jax.ShapeDtypeStruct(saved.shape, jnp.bfloat16),) + tuple(jax.ShapeDtypeStruct(w.shape, jnp.float32) for w in (w_1, w_2, w_3)),
        grid=(local, group),
        in_specs=[pl.BlockSpec(memory_space=pltpu.SMEM), by_pair((1, 1, 1, tokens)), by_pair((1, 1, 1, tokens)), pl.BlockSpec((1, tokens, model_dim), lambda e, p: (p, 0, 0)),
                  by_slot, by_expert((1, model_dim, ff)), by_expert((1, model_dim, ff)), by_expert((1, ff, model_dim))],
        out_specs=(by_slot, by_expert((1, model_dim, ff)), by_expert((1, ff, model_dim)), by_expert((1, model_dim, ff))),
        compiler_params=pltpu.CompilerParams(dimension_semantics=('arbitrary', 'arbitrary'), vmem_limit_bytes=VMEM_BYTES),
        cost_estimate=pl.CostEstimate(flops=group * local * capacity * model_dim * (2 * tokens + 16 * ff) // 2, bytes_accessed=saved.size * 4, transcendentals=0),
        name='experts_backward',
    )(counts, slot_rows[:, :, None, :], gate_rows[:, :, None, :], dy_rows, saved, w_1, w_3, w_2)


def combine_kernel(capacity, counts, slot_cols, buf_ref, out_ref):
    source = pl.program_id(0)
    tokens = out_ref.shape[1]
    out_ref[...] = jnp.zeros_like(out_ref)
    for expert in range(buf_ref.shape[0]):
        def body(size, expert=expert):
            cols = lax.broadcasted_iota(jnp.int32, (tokens, size), 1)
            mix = jnp.where(slot_cols[0, :, expert:expert + 1] == cols, 1.0, 0.0).astype(jnp.bfloat16)
            out_ref[0] += mm(mix, buf_ref[expert, :size, :])

        by_fill(counts[source, expert], capacity, body)


def combine_rows(counts, slot_cols, buf, capacity):
    group, tokens, local = slot_cols.shape
    model_dim = buf.shape[-1]
    return pl.pallas_call(
        functools.partial(combine_kernel, capacity),
        out_shape=jax.ShapeDtypeStruct((group, tokens, model_dim), jnp.float32),
        grid=(group,),
        in_specs=[pl.BlockSpec(memory_space=pltpu.SMEM), pl.BlockSpec((1, tokens, local), lambda p: (p, 0, 0)), pl.BlockSpec((local, capacity, model_dim), lambda p: (0, p, 0))],
        out_specs=pl.BlockSpec((1, tokens, model_dim), lambda p: (p, 0, 0)),
        compiler_params=pltpu.CompilerParams(dimension_semantics=('arbitrary',), vmem_limit_bytes=VMEM_BYTES),
        cost_estimate=pl.CostEstimate(flops=group * local * capacity * model_dim * tokens, bytes_accessed=group * tokens * model_dim * 8, transcendentals=0),
        name='combine_rows',
    )(counts, slot_cols, buf)


def lane_iota(shape):
    return lax.broadcasted_iota(jnp.int32, shape, len(shape) - 1)


def norm_rows(values, gain):
    scale = lax.rsqrt(jnp.mean(values * values, axis=-1, keepdims=True) + NORM_EPS)
    return values * scale, scale, (values * scale * gain).astype(jnp.bfloat16)


def norm_pull(values, gain, cotangent):
    scaled, scale, _ = norm_rows(values, gain)
    inner = cotangent * gain
    grad = scale * (inner - scaled * jnp.mean(inner * scaled, axis=-1, keepdims=True))
    return grad, jnp.sum(cotangent * scaled, axis=0, keepdims=True)


def project_kernel(score_scale, x_ref, gain_ref, w_ref, q_ref, k_ref, v_ref):
    normed = norm_rows(x_ref[...].astype(jnp.float32), gain_ref[...].astype(jnp.float32))[2]
    groups = q_ref.shape[0]
    width = q_ref.shape[2]
    mixed = round_bf16(mm(normed, w_ref[...]))
    for group in range(groups):
        q_ref[group] = (mixed[:, group * width:(group + 1) * width] * score_scale).astype(jnp.bfloat16)
    low = lane_iota((x_ref.shape[0], width)) < width // 2
    for start, ref in ((groups, k_ref), (groups * 3 // 2, v_ref)):
        for pair in range(groups // 2):
            both = mixed[:, (start + pair) * width:(start + pair + 1) * width]
            turned = pltpu.roll(both, width // 2, 1)
            ref[2 * pair] = jnp.where(low, both, turned).astype(jnp.bfloat16)
            ref[2 * pair + 1] = jnp.where(low, turned, both).astype(jnp.bfloat16)


def twin(rows, size):
    both = jnp.concatenate([rows, rows], axis=0)
    own = (lax.broadcasted_iota(jnp.int32, both.shape, 0) < size) == (lane_iota(both.shape) < both.shape[1] // 2)
    return jnp.where(own, both, jnp.zeros_like(both))


def untwin(columns, size):
    low = lax.broadcasted_iota(jnp.int32, (columns.shape[0], size), 0) < columns.shape[0] // 2
    return jnp.where(low, columns[:, :size], columns[:, size:]).T


def pieces(index, size):
    return ([(0, index * size)] if index else []) + [(index * size, (index + 1) * size)]


def causal_scores(k_ref, queries, start, stop, index, size):
    scores = mm(k_ref[0, start:stop, :], queries, NT)
    if start == index * size:
        column = lane_iota(scores.shape)
        row = lax.broadcasted_iota(jnp.int32, scores.shape, 0)
        scores = jnp.where(row <= jnp.where(column >= size, column - size, column), scores, -1e30)
    return scores


def attend_kernel(size, q_ref, k_ref, v_ref, out_ref, stat_ref):
    tokens = q_ref.shape[1]
    values_t = v_ref[0].T
    for index in range(tokens // size):
        rows = pl.ds(index * size, size)
        queries = twin(q_ref[0, rows, :], size)
        spans = pieces(index, size)
        scores = [causal_scores(k_ref, queries, a, b, index, size) for a, b in spans]
        top = functools.reduce(jnp.maximum, [jnp.max(part, axis=0, keepdims=True) for part in scores])
        exps = [jnp.exp(part - top) for part in scores]
        inverse = 1.0 / sum(jnp.sum(part, axis=0, keepdims=True) for part in exps)
        out = sum(mm(values_t[:, a:b], (part * inverse).astype(jnp.bfloat16)) for (a, b), part in zip(spans, exps))
        out_ref[0, rows, :] = untwin(out, size).astype(jnp.bfloat16)
        stat_ref[0, index, 0:1, :] = top
        stat_ref[0, index, 1:2, :] = inverse


def attend_pull_kernel(size, score_scale, q_ref, k_ref, v_ref, d_ref, stat_ref, dq_ref, dk_ref, dv_ref, dk_sum, dv_sum):
    tokens = q_ref.shape[1]
    width = q_ref.shape[2]
    keys_t = k_ref[0].T
    dk_sum[...] = jnp.zeros_like(dk_sum)
    dv_sum[...] = jnp.zeros_like(dv_sum)
    for index in range(tokens // size):
        rows = pl.ds(index * size, size)
        queries = twin(q_ref[0, rows, :], size)
        cotangent = twin(d_ref[0, rows, :], size)
        top = stat_ref[0, index, 0:1, :]
        inverse = stat_ref[0, index, 1:2, :]
        spans = pieces(index, size)
        probs, grads = [], []
        for a, b in spans:
            part = jnp.exp(causal_scores(k_ref, queries, a, b, index, size) - top) * inverse
            probs.append(part)
            dv_sum[a:b, :] += mm(part.astype(jnp.bfloat16), cotangent)
            grads.append(round_bf16(mm(v_ref[0, a:b, :], cotangent, NT)))
        inner = sum(jnp.sum(p * g, axis=0, keepdims=True) for p, g in zip(probs, grads))
        out = 0.0
        for (a, b), p, g in zip(spans, probs, grads):
            pull = (p * (g - inner)).astype(jnp.bfloat16)
            dk_sum[a:b, :] += mm(pull, queries)
            out = out + mm(keys_t[:, a:b], pull)
        dq_ref[0, rows, :] = (untwin(out, size) * score_scale).astype(jnp.bfloat16)
    dk_ref[0] = (dk_sum[...] + pltpu.roll(dk_sum[...], width // 2, 1)).astype(jnp.bfloat16)
    dv_ref[0] = (dv_sum[...] + pltpu.roll(dv_sum[...], width // 2, 1)).astype(jnp.bfloat16)


def merge_kernel(x_ref, gain_ref, ctx_ref, w_ref, h_ref, u_ref):
    context = jnp.concatenate([ctx_ref[group] for group in range(ctx_ref.shape[0])], axis=1)
    attn = round_bf16(mm(context, w_ref[...]))
    h_rows = (x_ref[...].astype(jnp.float32) + attn).astype(jnp.bfloat16)
    h_ref[...] = h_rows
    u_ref[...] = norm_rows(h_rows.astype(jnp.float32), gain_ref[...].astype(jnp.float32))[2]


def call(kernel, name, out_shape, flops, grid=(), **specs):
    return pl.pallas_call(
        kernel, out_shape=out_shape, grid=grid, name=name,
        compiler_params=pltpu.CompilerParams(dimension_semantics=('arbitrary',) * len(grid), vmem_limit_bytes=VMEM_BYTES),
        cost_estimate=pl.CostEstimate(flops=flops, bytes_accessed=2 ** 24, transcendentals=0), **specs)


def attention_forward(x, gain_1, gain_2, w_qkv, w_out, groups):
    tokens, model_dim = x.shape
    width = model_dim // groups
    block = tokens // 4
    heads = jax.ShapeDtypeStruct((groups, tokens, width), jnp.bfloat16)
    like = jax.ShapeDtypeStruct(x.shape, jnp.bfloat16)
    rows = pl.BlockSpec((block, model_dim), lambda i: (i, 0))
    head_rows = pl.BlockSpec((groups, block, width), lambda i: (0, i, 0))
    fixed = lambda array: pl.BlockSpec(array.shape, lambda i: (0, 0))
    query, key, value = call(functools.partial(project_kernel, (width // 2) ** -0.5), 'project', (heads,) * 3, 4 * tokens * model_dim ** 2, (4,),
                             in_specs=[rows, fixed(gain_1), fixed(w_qkv)], out_specs=(head_rows,) * 3)(x, gain_1, w_qkv)
    head = pl.BlockSpec((1, tokens, width), lambda g: (g, 0, 0))
    stat_shape = (groups, 4, 2, 2 * block)
    stat = pl.BlockSpec((1,) + stat_shape[1:], lambda g: (g, 0, 0, 0))
    context, stats = call(functools.partial(attend_kernel, block), 'attend', (heads, jax.ShapeDtypeStruct(stat_shape, jnp.float32)), 16 * tokens ** 2 * model_dim, (groups,),
                          in_specs=[head] * 3, out_specs=(head, stat))(query, key, value)
    h_rows, u_rows = call(merge_kernel, 'merge', (like, like), 2 * tokens * model_dim ** 2, (4,),
                          in_specs=[rows, fixed(gain_2), head_rows, fixed(w_out)], out_specs=(rows, rows))(x, gain_2, context, w_out)
    return h_rows, u_rows, (query, key, value, context, stats)


def out_pull_kernel(h_ref, dy_ref, du_ref, gain_ref, ctx_ref, w_ref, dh_ref, dctx_ref, grad_o_ref, grad_n_ref):
    groups, tokens, width = ctx_ref.shape
    gain = gain_ref[...].astype(jnp.float32)
    block = tokens // 4
    total = 0.0
    for index in range(4):
        rows = pl.ds(index * block, block)
        grad, part = norm_pull(h_ref[rows, :].astype(jnp.float32), gain, round_bf16(du_ref[rows, :]))
        total = total + part
        d_rows = (dy_ref[rows, :].astype(jnp.float32) + round_bf16(grad)).astype(jnp.bfloat16)
        dh_ref[rows, :] = d_rows
        pulled = mm(d_rows, w_ref[...], NT).astype(jnp.bfloat16)
        for group in range(groups):
            dctx_ref[group, rows, :] = pulled[:, group * width:(group + 1) * width]
    grad_n_ref[...] = round_bf16(total)
    for group in range(0, groups, 2):
        context = jnp.concatenate([ctx_ref[group], ctx_ref[group + 1]], axis=1)
        grad_o_ref[group * width:(group + 2) * width, :] = round_bf16(mm(context, dh_ref[...], TN))


def in_pull_kernel(x_ref, dh_ref, dq_ref, dk_ref, dv_ref, gain_ref, w_ref, dx_ref, gq_ref, gk_ref, gv_ref, gn_ref, normed_ref, mixed_ref):
    groups, tokens, width = dq_ref.shape
    model_dim = x_ref.shape[1]
    gain = gain_ref[...].astype(jnp.float32)
    block = tokens // 4
    low = lane_iota((block, width)) < width // 2
    total = 0.0
    for index in range(4):
        rows = pl.ds(index * block, block)
        for group in range(groups):
            mixed_ref[rows, group * width:(group + 1) * width] = dq_ref[group, rows, :]
        for start, ref in ((groups, dk_ref), (groups * 3 // 2, dv_ref)):
            for pair in range(groups // 2):
                mixed_ref[rows, (start + pair) * width:(start + pair + 1) * width] = jnp.where(low, ref[2 * pair, rows, :], ref[2 * pair + 1, rows, :])
        values = x_ref[rows, :].astype(jnp.float32)
        normed_ref[rows, :] = norm_rows(values, gain)[2]
        grad, part = norm_pull(values, gain, round_bf16(mm(mixed_ref[rows, :], w_ref[...], NT)))
        total = total + part
        dx_ref[rows, :] = (dh_ref[rows, :].astype(jnp.float32) + round_bf16(grad)).astype(jnp.bfloat16)
    gn_ref[...] = round_bf16(total)
    half = model_dim // 2
    for start, ref in ((0, gq_ref), (2, gk_ref), (3, gv_ref)):
        for part in range(ref.shape[1] // half):
            ref[:, part * half:(part + 1) * half] = round_bf16(mm(normed_ref[...], mixed_ref[:, (start + part) * half:(start + part + 1) * half], TN))


def attention_backward(x, dy, du, h_rows, saved, gain_1, gain_2, w_qkv, w_out):
    query, key, value, context, stats = saved
    groups, tokens, width = query.shape
    model_dim = x.shape[1]
    heads = jax.ShapeDtypeStruct(query.shape, jnp.bfloat16)
    like = jax.ShapeDtypeStruct(x.shape, jnp.bfloat16)
    wide = lambda *shape: jax.ShapeDtypeStruct(shape, jnp.float32)
    dh, d_context, grad_o, grad_n2 = call(out_pull_kernel, 'out_pull', (like, heads, wide(model_dim, model_dim), wide(1, model_dim)), 4 * tokens * model_dim ** 2)(
        h_rows, dy, du, gain_2, context, w_out)
    head = pl.BlockSpec((1, tokens, width), lambda g: (g, 0, 0))
    stat = pl.BlockSpec((1,) + stats.shape[1:], lambda g: (g, 0, 0, 0))
    d_query, d_key, d_value = call(functools.partial(attend_pull_kernel, tokens // 4, (width // 2) ** -0.5), 'attend_pull', (heads,) * 3, 40 * tokens ** 2 * model_dim, (groups,),
                                   in_specs=[head] * 4 + [stat], out_specs=(head,) * 3, scratch_shapes=[pltpu.VMEM((tokens, width), jnp.float32)] * 2)(query, key, value, d_context, stats)
    dx, grad_q, grad_k, grad_v, grad_n1 = call(
        in_pull_kernel, 'in_pull', (like, wide(model_dim, model_dim), wide(model_dim, model_dim // 2), wide(model_dim, model_dim // 2), wide(1, model_dim)), 8 * tokens * model_dim ** 2,
        scratch_shapes=[pltpu.VMEM((tokens, model_dim), jnp.bfloat16), pltpu.VMEM((tokens, 2 * model_dim), jnp.bfloat16)])(x, dh, d_query, d_key, d_value, gain_1, w_qkv)
    return dx, grad_q, grad_k, grad_v, grad_o, grad_n1, grad_n2


def solution(mesh):
    group = mesh.shape['expert']

    def local_step(x_a, x_b, dy_b, eid_a, slot_a, gate_a, eid_b, slot_b, gate_b, u_b, norm_1, norm_2, w_q, w_k, w_v, w_o, w_1, w_2, w_3):
        local_experts = w_1.shape[0]
        experts = local_experts * group
        capacity = u_b.shape[1] // group
        model_dim = x_a.shape[1]

        tokens = x_a.shape[0]
        meta = jnp.stack([*expert_map(eid_a, slot_a, gate_a, experts), *expert_map(eid_b, slot_b, gate_b, experts)], axis=1)
        meta = lax.all_to_all(meta.reshape(group, local_experts, 4, tokens), 'expert', 0, 0, tiled=True)
        slots_a, gates_a, slots_b, gates_b = (meta[:, :, i] for i in range(4))
        rows_a, rows_b = slots_a.astype(jnp.int32), slots_b.astype(jnp.int32)
        counts_a, counts_b = (jnp.sum((rows >= 0).astype(jnp.int32), axis=2) for rows in (rows_a, rows_b))
        cols_a, cols_b = jnp.swapaxes(rows_a, 1, 2), jnp.swapaxes(rows_b, 1, 2)

        all_dy = lax.all_gather(dy_b, 'expert', axis=0, tiled=True).reshape(group, tokens, model_dim)
        kv_heads = w_k.shape[1]
        w_qkv = jnp.concatenate([w_q.reshape(model_dim, -1), w_k.reshape(model_dim, -1), w_v.reshape(model_dim, -1)], axis=1)
        w_out = w_o.reshape(-1, model_dim)
        gain_1, gain_2 = norm_1[None], norm_2[None]
        h_a, u_a, _ = attention_forward(x_a, gain_1, gain_2, w_qkv, w_out, kv_heads)
        all_u = lax.all_gather(u_a, 'expert', axis=0, tiled=True).reshape(group, tokens, model_dim)
        h_b, _, kept_b = attention_forward(x_b, gain_1, gain_2, w_qkv, w_out, kv_heads)

        grad_in, grad_w1, grad_w2, grad_w3 = experts_backward(counts_b, rows_b, gates_b, all_dy, u_b, w_1, w_3, w_2, capacity)
        part_b = combine_rows(counts_b, cols_b, grad_in, capacity)
        du_rows = lax.psum_scatter(part_b.reshape(group * tokens, model_dim), 'expert', scatter_dimension=0, tiled=True)

        part_a = experts_forward(counts_a, rows_a, cols_a, jnp.swapaxes(gates_a, 1, 2), all_u, w_1, w_3, w_2, capacity)
        mixed = lax.psum_scatter(part_a.reshape(group * tokens, model_dim), 'expert', scatter_dimension=0, tiled=True)
        y_a = (h_a.astype(jnp.float32) + mixed).astype(jnp.bfloat16)
        dx_b, g_q, g_k, g_v, g_o, g_n1, g_n2 = attention_backward(x_b, dy_b, du_rows, h_b, kept_b, gain_1, gain_2, w_qkv, w_out)
        return (y_a, dx_b, grad_w1, grad_w2, grad_w3, g_q.reshape((1,) + w_q.shape), g_k.reshape((1,) + w_k.shape), g_v.reshape((1,) + w_v.shape), g_o.reshape((1,) + w_o.shape), g_n1, g_n2)

    row_spec = P(('data', 'expert'), None)
    cube_spec = P(('data', 'expert'), None, None)
    quad_spec = P(('data', 'expert'), None, None, None)
    expert_spec = P('expert', None, None)
    in_specs = (row_spec, row_spec, row_spec, row_spec, row_spec, row_spec, row_spec, row_spec, row_spec, cube_spec, P(), P(), P(), P(), P(), P(), expert_spec, expert_spec, expert_spec)
    out_specs = (row_spec, row_spec, cube_spec, cube_spec, cube_spec, quad_spec, quad_spec, quad_spec, quad_spec, row_spec, row_spec)
    return jax.shard_map(local_step, mesh=mesh, in_specs=in_specs, out_specs=out_specs, check_vma=False)
```

```python
import functools

import jax
import jax.numpy as jnp
from jax import lax
from jax.experimental import pallas as pl
from jax.experimental.pallas import tpu as pltpu
from jax.sharding import PartitionSpec as P

NORM_EPS = 1e-6


def expert_map(expert_ids, slot_ids, gates, chosen):
    held = (expert_ids[None] == chosen[:, None, None]) & (slot_ids >= 0)[None]
    slot_map = jnp.max(jnp.where(held, slot_ids[None], -1), axis=2).astype(jnp.float32)
    gate_map = jnp.sum(jnp.where(held, gates.astype(jnp.float32)[None], 0.0), axis=2)
    return slot_map, gate_map


def swap(values, mask, group):
    return lax.ppermute(values, 'expert', [(i, i ^ mask) for i in range(group)])


VMEM_BYTES = 60 * 2 ** 20
NT = (((1,), (1,)), ((), ()))
TN = (((0,), (0,)), ((), ()))


def mm(lhs, rhs, dims=(((1,), (0,)), ((), ()))):
    return lax.dot_general(lhs, rhs, dims, preferred_element_type=jnp.float32)


def round_bf16(values):
    return values.astype(jnp.bfloat16).astype(jnp.float32)


def fill_sizes(capacity):
    return (capacity * 17 // 32 // 16 * 16, capacity)


def by_fill(count, capacity, body):
    low = 0
    for size in fill_sizes(capacity):
        pl.when((count > low) & (count <= size))(functools.partial(body, size))
        low = size


def pair_maps(meta_ref, first):
    rows = meta_ref[0, 0]
    cols = jnp.concatenate([rows, rows], axis=0).T
    return rows[first:first + 1].astype(jnp.int32), rows[first + 1:first + 2], cols[:, first:first + 1].astype(jnp.int32), cols[:, first + 1:first + 2]


def select_rows(slot, values, size):
    rows = lax.broadcasted_iota(jnp.int32, (size, slot.shape[1]), 0)
    return jnp.where(slot == rows, values, 0.0).astype(jnp.bfloat16)


def select_cols(slot, values, size):
    cols = lax.broadcasted_iota(jnp.int32, (slot.shape[0], size), 1)
    return jnp.where(slot == cols, values, 0.0).astype(jnp.bfloat16)


def forward_kernel(capacity, bit, counts, order, meta_ref, x_ref, w1_ref, w3_ref, w2_ref, *refs):
    out_ref = refs[-1]
    place, expert = pl.program_id(0), pl.program_id(1)

    @pl.when(expert == 0)
    def _():
        out_ref[...] = refs[0][...] if len(refs) > 1 else jnp.zeros_like(out_ref)

    def body(size):
        slot_row, _, slot_col, gate_col = pair_maps(meta_ref, 0)
        buf = mm(select_rows(slot_row, 1.0, size), x_ref[0]).astype(jnp.bfloat16)
        act_1 = round_bf16(mm(buf, w1_ref[expert]))
        act_3 = round_bf16(mm(buf, w3_ref[expert]))
        hidden = (act_1 * jax.nn.sigmoid(act_1) * act_3).astype(jnp.bfloat16)
        out = mm(hidden, w2_ref[expert]).astype(jnp.bfloat16)
        out_ref[0] += mm(select_cols(slot_col, gate_col, size), out)

    by_fill(counts[order[1, 2 * place + bit], expert], capacity, body)


def backward_kernel(capacity, bit, counts, order, meta_ref, dy_ref, u_ref, w1_ref, w3_ref, w2_ref, out_ref, d_ref, hid_ref, a1_ref, a3_ref):
    place, expert = pl.program_id(0), pl.program_id(1)

    @pl.when(expert == 0)
    def _():
        out_ref[...] = jnp.zeros_like(out_ref)

    def body(size):
        slot_row, gate_row, slot_col, _ = pair_maps(meta_ref, 2)
        d_out = mm(select_rows(slot_row, gate_row, size), dy_ref[0]).astype(jnp.bfloat16)
        d_ref[0, :size, :] = d_out
        saved = u_ref[0, :size, :]
        pre_1 = round_bf16(mm(saved, w1_ref[expert]))
        pre_3 = round_bf16(mm(saved, w3_ref[expert]))
        sigma = jax.nn.sigmoid(pre_1)
        silu_1 = pre_1 * sigma
        hid_ref[0, :size, :] = (silu_1 * pre_3).astype(jnp.bfloat16)
        grad_hid = round_bf16(mm(d_out, w2_ref[expert], NT))
        grad_a1 = (grad_hid * pre_3 * sigma * (1.0 + pre_1 * (1.0 - sigma))).astype(jnp.bfloat16)
        grad_a3 = (grad_hid * silu_1).astype(jnp.bfloat16)
        a1_ref[0, :size, :] = grad_a1
        a3_ref[0, :size, :] = grad_a3
        grad_in = (mm(grad_a1, w1_ref[expert], NT) + mm(grad_a3, w3_ref[expert], NT)).astype(jnp.bfloat16)
        out_ref[0] += mm(select_cols(slot_col, 1.0, size), grad_in)

    by_fill(counts[order[1, 2 * place + bit], expert], capacity, body)


def weights_kernel(capacity, counts, order, *refs):
    expert, place = pl.program_id(0), pl.program_id(1)
    g1_ref, g2_ref, g3_ref = refs[10:]

    @pl.when(place == 0)
    def _():
        g1_ref[...] = jnp.zeros_like(g1_ref)
        g2_ref[...] = jnp.zeros_like(g2_ref)
        g3_ref[...] = jnp.zeros_like(g3_ref)

    for bit in range(2):
        u_ref, d_ref, hid_ref, a1_ref, a3_ref = refs[5 * bit:5 * bit + 5]

        def body(size):
            g2_ref[0] += mm(hid_ref[0, :size, :], d_ref[0, :size, :], TN)
            g1_ref[0] += mm(u_ref[0, :size, :], a1_ref[0, :size, :], TN)
            g3_ref[0] += mm(u_ref[0, :size, :], a3_ref[0, :size, :], TN)

        by_fill(counts[order[1, 2 * place + bit], expert], capacity, body)


def ordered_call(kernel, name, out_shape, flops, grid, in_specs, out_specs):
    return pl.pallas_call(
        kernel, out_shape=out_shape, name=name,
        grid_spec=pltpu.PrefetchScalarGridSpec(num_scalar_prefetch=2, grid=grid, in_specs=in_specs, out_specs=out_specs),
        compiler_params=pltpu.CompilerParams(dimension_semantics=('arbitrary',) * len(grid), vmem_limit_bytes=VMEM_BYTES),
        cost_estimate=pl.CostEstimate(flops=flops, bytes_accessed=2 ** 24, transcendentals=0))


def pair_specs(bit, meta, rows, weights):
    pair = pl.BlockSpec((1, 1) + meta.shape[2:], lambda i, e, counts, order: (order[1, 2 * i + bit], e, 0, 0))
    source = pl.BlockSpec((1,) + rows.shape[1:], lambda i, e, counts, order: (order[0, 2 * i + bit], 0, 0))
    whole = [pl.BlockSpec(w.shape, lambda i, e, counts, order: (0, 0, 0), pipeline_mode=pl.Buffered(1)) for w in weights]
    part = pl.BlockSpec((1,) + rows.shape[1:], lambda i, e, counts, order: (i, 0, 0))
    return pair, source, whole, part


def experts_forward(bit, counts, order, meta, rows, weights, capacity, *start):
    group, tokens, model_dim = rows.shape
    local, _, ff = weights[0].shape
    pair, source, whole, part = pair_specs(bit, meta, rows, weights)
    return ordered_call(functools.partial(forward_kernel, capacity, bit), 'experts_forward', jax.ShapeDtypeStruct((group // 2, tokens, model_dim), jnp.float32),
                        group * local * capacity * model_dim * (4 * tokens + 6 * ff) // 4, (group // 2, local), [pair, source] + whole + [part] * len(start), part)(counts, order, meta, rows, *weights, *start)


def experts_backward(bit, counts, order, meta, rows, saved, weights, capacity):
    group, tokens, model_dim = rows.shape
    local, _, ff = weights[0].shape
    pair, source, whole, part = pair_specs(bit, meta, rows, weights)
    stored = pl.BlockSpec((1, capacity, model_dim), lambda i, e, counts, order: (e, order[0, 2 * i + bit], 0))
    slots = lambda width: pl.BlockSpec((1, capacity, width), lambda i, e, counts, order: (e, i, 0))
    kept = lambda width: jax.ShapeDtypeStruct((local, group // 2 * capacity, width), jnp.bfloat16)
    return ordered_call(functools.partial(backward_kernel, capacity, bit), 'experts_backward',
                        (jax.ShapeDtypeStruct((group // 2, tokens, model_dim), jnp.float32), kept(model_dim), kept(ff), kept(ff), kept(ff)),
                        group * local * capacity * model_dim * (4 * tokens + 10 * ff) // 4, (group // 2, local),
                        [pair, source, stored] + whole, (part, slots(model_dim), slots(ff), slots(ff), slots(ff)))(counts, order, meta, rows, saved, *weights)


def experts_weights(counts, order, saved, kept_near, kept_far, capacity):
    local, slots_all, model_dim = saved.shape
    ff = kept_near[1].shape[2]
    slots = lambda width: pl.BlockSpec((1, capacity, width), lambda e, i, counts, order: (e, i, 0))
    stored = lambda bit: pl.BlockSpec((1, capacity, model_dim), lambda e, i, counts, order: (e, order[0, 2 * i + bit], 0))
    shapes = ((model_dim, ff), (ff, model_dim), (model_dim, ff))
    inner = [slots(model_dim), slots(ff), slots(ff), slots(ff)]
    return ordered_call(functools.partial(weights_kernel, capacity), 'experts_weights', tuple(jax.ShapeDtypeStruct((local,) + shape, jnp.float32) for shape in shapes),
                        local * slots_all * model_dim * 6 * ff // 2, (local, slots_all // capacity // 2),
                        [stored(0)] + inner + [stored(1)] + inner,
                        tuple(pl.BlockSpec((1,) + shape, lambda e, i, counts, order: (e, 0, 0)) for shape in shapes))(counts, order, saved, *kept_near, saved, *kept_far)


def lane_iota(shape):
    return lax.broadcasted_iota(jnp.int32, shape, len(shape) - 1)


def norm_rows(values, gain):
    scale = lax.rsqrt(jnp.mean(values * values, axis=-1, keepdims=True) + NORM_EPS)
    return values * scale, scale, (values * scale * gain).astype(jnp.bfloat16)


def norm_pull(values, gain, cotangent):
    scaled, scale, _ = norm_rows(values, gain)
    inner = cotangent * gain
    grad = scale * (inner - scaled * jnp.mean(inner * scaled, axis=-1, keepdims=True))
    return grad, jnp.sum(cotangent * scaled, axis=0, keepdims=True)


def project_kernel(score_scale, x_ref, gain_ref, w_ref, q_ref, k_ref, v_ref):
    normed = norm_rows(x_ref[...].astype(jnp.float32), gain_ref[...].astype(jnp.float32))[2]
    groups = q_ref.shape[0]
    width = q_ref.shape[2]
    mixed = round_bf16(mm(normed, w_ref[...], NT))
    for group in range(groups):
        q_ref[group] = (mixed[:, group * width:(group + 1) * width] * score_scale).astype(jnp.bfloat16)
    low = lane_iota((x_ref.shape[0], width)) < width // 2
    for start, ref in ((groups, k_ref), (groups * 3 // 2, v_ref)):
        for pair in range(groups // 2):
            both = mixed[:, (start + pair) * width:(start + pair + 1) * width]
            turned = pltpu.roll(both, width // 2, 1)
            ref[2 * pair] = jnp.where(low, both, turned).astype(jnp.bfloat16)
            ref[2 * pair + 1] = jnp.where(low, turned, both).astype(jnp.bfloat16)


def twin(rows, size):
    both = jnp.concatenate([rows, rows], axis=0)
    own = (lax.broadcasted_iota(jnp.int32, both.shape, 0) < size) == (lane_iota(both.shape) < both.shape[1] // 2)
    return jnp.where(own, both, jnp.zeros_like(both))


def untwin(columns, size):
    low = lax.broadcasted_iota(jnp.int32, (columns.shape[0], size), 0) < columns.shape[0] // 2
    return jnp.where(low, columns[:, :size], columns[:, size:]).T


def pieces(index, size):
    return ([(0, index * size)] if index else []) + [(index * size, (index + 1) * size)]


def causal_scores(k_ref, queries, start, stop, index, size):
    scores = mm(k_ref[0, start:stop, :], queries, NT)
    if start == index * size:
        column = lane_iota(scores.shape)
        row = lax.broadcasted_iota(jnp.int32, scores.shape, 0)
        scores = jnp.where(row <= jnp.where(column >= size, column - size, column), scores, -1e30)
    return scores


def attend_kernel(size, q_ref, k_ref, v_ref, out_ref, stat_ref):
    tokens = q_ref.shape[1]
    values_t = v_ref[0].T
    for index in range(tokens // size):
        rows = pl.ds(index * size, size)
        queries = twin(q_ref[0, rows, :], size)
        spans = pieces(index, size)
        scores = [causal_scores(k_ref, queries, a, b, index, size) for a, b in spans]
        top = functools.reduce(jnp.maximum, [jnp.max(part, axis=0, keepdims=True) for part in scores])
        exps = [jnp.exp(part - top) for part in scores]
        inverse = 1.0 / sum(jnp.sum(part, axis=0, keepdims=True) for part in exps)
        out = sum(mm(values_t[:, a:b], (part * inverse).astype(jnp.bfloat16)) for (a, b), part in zip(spans, exps))
        out_ref[0, rows, :] = untwin(out, size).astype(jnp.bfloat16)
        stat_ref[0, index, 0:1, :] = top
        stat_ref[0, index, 1:2, :] = inverse


def attend_pull_kernel(size, score_scale, q_ref, k_ref, v_ref, d_ref, stat_ref, dq_ref, dk_ref, dv_ref, dk_sum, dv_sum):
    tokens = q_ref.shape[1]
    width = q_ref.shape[2]
    keys_t = k_ref[0].T
    dk_sum[...] = jnp.zeros_like(dk_sum)
    dv_sum[...] = jnp.zeros_like(dv_sum)
    for index in range(tokens // size):
        rows = pl.ds(index * size, size)
        queries = twin(q_ref[0, rows, :], size)
        cotangent = twin(d_ref[0, rows, :], size)
        top = stat_ref[0, index, 0:1, :]
        inverse = stat_ref[0, index, 1:2, :]
        spans = pieces(index, size)
        probs, grads = [], []
        for a, b in spans:
            part = jnp.exp(causal_scores(k_ref, queries, a, b, index, size) - top) * inverse
            probs.append(part)
            dv_sum[a:b, :] += mm(part.astype(jnp.bfloat16), cotangent)
            grads.append(round_bf16(mm(v_ref[0, a:b, :], cotangent, NT)))
        inner = sum(jnp.sum(p * g, axis=0, keepdims=True) for p, g in zip(probs, grads))
        out = 0.0
        for (a, b), p, g in zip(spans, probs, grads):
            pull = (p * (g - inner)).astype(jnp.bfloat16)
            dk_sum[a:b, :] += mm(pull, queries)
            out = out + mm(keys_t[:, a:b], pull)
        dq_ref[0, rows, :] = (untwin(out, size) * score_scale).astype(jnp.bfloat16)
    dk_ref[0] = (dk_sum[...] + pltpu.roll(dk_sum[...], width // 2, 1)).astype(jnp.bfloat16)
    dv_ref[0] = (dv_sum[...] + pltpu.roll(dv_sum[...], width // 2, 1)).astype(jnp.bfloat16)


def merge_kernel(x_ref, gain_ref, ctx_ref, w_ref, h_ref, u_ref):
    context = jnp.concatenate([ctx_ref[group] for group in range(ctx_ref.shape[0])], axis=1)
    attn = round_bf16(mm(context, w_ref[...]))
    h_rows = (x_ref[...].astype(jnp.float32) + attn).astype(jnp.bfloat16)
    h_ref[...] = h_rows
    u_ref[...] = norm_rows(h_rows.astype(jnp.float32), gain_ref[...].astype(jnp.float32))[2]


def call(kernel, name, out_shape, flops, grid=(), **specs):
    return pl.pallas_call(
        kernel, out_shape=out_shape, grid=grid, name=name,
        compiler_params=pltpu.CompilerParams(dimension_semantics=('arbitrary',) * len(grid), vmem_limit_bytes=VMEM_BYTES),
        cost_estimate=pl.CostEstimate(flops=flops, bytes_accessed=2 ** 24, transcendentals=0), **specs)


def project(x, gain_1, w_qkv, groups):
    tokens, model_dim = x.shape
    width = model_dim // groups
    block = tokens // 4
    rows = pl.BlockSpec((block, model_dim), lambda i: (i, 0))
    head_rows = pl.BlockSpec((groups, block, width), lambda i: (0, i, 0))
    fixed = lambda array: pl.BlockSpec(array.shape, lambda i: (0, 0))
    return call(functools.partial(project_kernel, (width // 2) ** -0.5), 'project', (jax.ShapeDtypeStruct((groups, tokens, width), jnp.bfloat16),) * 3, 4 * tokens * model_dim ** 2, (4,),
                in_specs=[rows, fixed(gain_1), fixed(w_qkv)], out_specs=(head_rows,) * 3)(x, gain_1, w_qkv)


def attention_forward(x, projected, gain_2, w_out):
    query, key, value = projected
    groups, tokens, width = query.shape
    model_dim = x.shape[1]
    block = tokens // 4
    heads = jax.ShapeDtypeStruct(query.shape, jnp.bfloat16)
    like = jax.ShapeDtypeStruct(x.shape, jnp.bfloat16)
    rows = pl.BlockSpec((block, model_dim), lambda i: (i, 0))
    head_rows = pl.BlockSpec((groups, block, width), lambda i: (0, i, 0))
    fixed = lambda array: pl.BlockSpec(array.shape, lambda i: (0, 0))
    head = pl.BlockSpec((1, tokens, width), lambda g: (g, 0, 0))
    stat_shape = (groups, 4, 2, 2 * block)
    stat = pl.BlockSpec((1,) + stat_shape[1:], lambda g: (g, 0, 0, 0))
    context, stats = call(functools.partial(attend_kernel, block), 'attend', (heads, jax.ShapeDtypeStruct(stat_shape, jnp.float32)), 16 * tokens ** 2 * model_dim, (groups,),
                          in_specs=[head] * 3, out_specs=(head, stat))(query, key, value)
    h_rows, u_rows = call(merge_kernel, 'merge', (like, like), 2 * tokens * model_dim ** 2, (4,),
                          in_specs=[rows, fixed(gain_2), head_rows, fixed(w_out)], out_specs=(rows, rows))(x, gain_2, context, w_out)
    return h_rows, u_rows, (query, key, value, context, stats)


def out_pull_kernel(h_ref, dy_ref, du_ref, gain_ref, ctx_ref, w_ref, dh_ref, dctx_ref, grad_o_ref, grad_n_ref):
    groups, tokens, width = ctx_ref.shape
    gain = gain_ref[...].astype(jnp.float32)
    block = tokens // 4
    total = 0.0
    for index in range(4):
        rows = pl.ds(index * block, block)
        grad, part = norm_pull(h_ref[rows, :].astype(jnp.float32), gain, round_bf16(du_ref[rows, :]))
        total = total + part
        d_rows = (dy_ref[rows, :].astype(jnp.float32) + round_bf16(grad)).astype(jnp.bfloat16)
        dh_ref[rows, :] = d_rows
        pulled = mm(d_rows, w_ref[...], NT).astype(jnp.bfloat16)
        for group in range(groups):
            dctx_ref[group, rows, :] = pulled[:, group * width:(group + 1) * width]
    grad_n_ref[...] = round_bf16(total)
    for group in range(0, groups, 2):
        context = jnp.concatenate([ctx_ref[group], ctx_ref[group + 1]], axis=1)
        grad_o_ref[group * width:(group + 2) * width, :] = round_bf16(mm(context, dh_ref[...], TN))


def in_pull_kernel(x_ref, dh_ref, dq_ref, dk_ref, dv_ref, gain_ref, w_ref, dx_ref, gq_ref, gk_ref, gv_ref, gn_ref, normed_ref, mixed_ref):
    groups, tokens, width = dq_ref.shape
    model_dim = x_ref.shape[1]
    gain = gain_ref[...].astype(jnp.float32)
    block = tokens // 4
    low = lane_iota((block, width)) < width // 2
    total = 0.0
    for index in range(4):
        rows = pl.ds(index * block, block)
        for group in range(groups):
            mixed_ref[rows, group * width:(group + 1) * width] = dq_ref[group, rows, :]
        for start, ref in ((groups, dk_ref), (groups * 3 // 2, dv_ref)):
            for pair in range(groups // 2):
                mixed_ref[rows, (start + pair) * width:(start + pair + 1) * width] = jnp.where(low, ref[2 * pair, rows, :], ref[2 * pair + 1, rows, :])
        values = x_ref[rows, :].astype(jnp.float32)
        normed_ref[rows, :] = norm_rows(values, gain)[2]
        grad, part = norm_pull(values, gain, round_bf16(mm(mixed_ref[rows, :], w_ref[...])))
        total = total + part
        dx_ref[rows, :] = (dh_ref[rows, :].astype(jnp.float32) + round_bf16(grad)).astype(jnp.bfloat16)
    gn_ref[...] = round_bf16(total)
    half = model_dim // 2
    for start, ref in ((0, gq_ref), (2, gk_ref), (3, gv_ref)):
        for part in range(ref.shape[0] // half):
            ref[part * half:(part + 1) * half, :] = round_bf16(mm(mixed_ref[:, (start + part) * half:(start + part + 1) * half], normed_ref[...], TN))


def attention_pull(dy, du, h_rows, saved, gain_2, w_out):
    query, key, value, context, stats = saved
    groups, tokens, width = query.shape
    model_dim = dy.shape[1]
    heads = jax.ShapeDtypeStruct(query.shape, jnp.bfloat16)
    like = jax.ShapeDtypeStruct(dy.shape, jnp.bfloat16)
    wide = lambda *shape: jax.ShapeDtypeStruct(shape, jnp.float32)
    dh, d_context, grad_o, grad_n2 = call(out_pull_kernel, 'out_pull', (like, heads, wide(model_dim, model_dim), wide(1, model_dim)), 4 * tokens * model_dim ** 2)(
        h_rows, dy, du, gain_2, context, w_out)
    head = pl.BlockSpec((1, tokens, width), lambda g: (g, 0, 0))
    stat = pl.BlockSpec((1,) + stats.shape[1:], lambda g: (g, 0, 0, 0))
    d_query, d_key, d_value = call(functools.partial(attend_pull_kernel, tokens // 4, (width // 2) ** -0.5), 'attend_pull', (heads,) * 3, 40 * tokens ** 2 * model_dim, (groups,),
                                   in_specs=[head] * 4 + [stat], out_specs=(head,) * 3, scratch_shapes=[pltpu.VMEM((tokens, width), jnp.float32)] * 2)(query, key, value, d_context, stats)
    return dh, grad_o, grad_n2, (d_query, d_key, d_value)


def projection_pull(x, dh, pulls, gain_1, w_qkv):
    tokens, model_dim = x.shape
    like = jax.ShapeDtypeStruct(x.shape, jnp.bfloat16)
    wide = lambda *shape: jax.ShapeDtypeStruct(shape, jnp.float32)
    return call(
        in_pull_kernel, 'in_pull', (like, wide(model_dim, model_dim), wide(model_dim // 2, model_dim), wide(model_dim // 2, model_dim), wide(1, model_dim)), 8 * tokens * model_dim ** 2,
        scratch_shapes=[pltpu.VMEM((tokens, model_dim), jnp.bfloat16), pltpu.VMEM((tokens, 2 * model_dim), jnp.bfloat16)])(x, dh, *pulls, gain_1, w_qkv)


def solution(mesh):
    group = mesh.shape['expert']

    def local_step(x_a, x_b, dy_b, eid_a, slot_a, gate_a, eid_b, slot_b, gate_b, u_b, norm_1, norm_2, w_q, w_k, w_v, w_o, w_1, w_2, w_3):
        local_experts = w_1.shape[0]
        experts = local_experts * group
        capacity = u_b.shape[1] // group
        model_dim = x_a.shape[1]

        tokens = x_a.shape[0]
        me = lax.axis_index('expert')
        turned = me ^ jnp.arange(group, dtype=jnp.int32)
        places = (me % 2) ^ jnp.arange(group, dtype=jnp.int32)
        order = jnp.stack([places, places ^ me])
        chosen = (turned[:, None] * local_experts + jnp.arange(local_experts, dtype=jnp.int32)[None, :]).reshape(-1)
        meta = jnp.stack([*expert_map(eid_a, slot_a, gate_a, chosen), *expert_map(eid_b, slot_b, gate_b, chosen)], axis=1)
        meta = meta.reshape(group, local_experts, 4, tokens)
        meta = jnp.stack([meta[0]] + [swap(meta[r], r, group) for r in range(1, group)])
        counts_a, counts_b = (jnp.sum((meta[:, :, i] >= 0).astype(jnp.int32), axis=2) for i in (0, 2))
        weights = (w_1, w_3, w_2)

        all_dy = lax.all_gather(dy_b, 'expert', axis=0, tiled=True).reshape(group, tokens, model_dim)
        kv_heads = w_k.shape[1]
        w_qkv = jnp.concatenate([w.reshape(model_dim, -1).T for w in (w_q, w_k, w_v)], axis=0)
        w_out = w_o.reshape(-1, model_dim)
        gain_1, gain_2 = norm_1[None], norm_2[None]
        h_a, u_a, _ = attention_forward(x_a, project(x_a, gain_1, w_qkv, kv_heads), gain_2, w_out)
        all_u = lax.all_gather(u_a, 'expert', axis=0, tiled=True).reshape(group, tokens, model_dim)
        all_dy, projected_b = lax.optimization_barrier((all_dy, project(x_b, gain_1, w_qkv, kv_heads)))
        same_core = [[i for i in range(group) if i % 2 == core] for core in range(2)]
        reduce_chips = lambda part: lax.psum_scatter(part.reshape(-1, model_dim), 'expert', scatter_dimension=0, tiled=True, axis_index_groups=same_core)
        far_b, *kept_far = experts_backward(1, counts_b, order, meta, all_dy, u_b, weights, capacity)
        far_b, all_dy = lax.optimization_barrier((far_b, all_dy))
        came_b = swap(far_b, 1, group)
        near_b, *kept_near = experts_backward(0, counts_b, order, meta, all_dy, u_b, weights, capacity)
        part_b, all_u, kept_near = lax.optimization_barrier((near_b + came_b, all_u, kept_near))
        du_rows = reduce_chips(part_b)
        far_a = experts_forward(1, counts_a, order, meta, all_u, weights, capacity)
        far_a, projected_b, all_u = lax.optimization_barrier((far_a, projected_b, all_u))
        came_a = swap(far_a, 1, group)
        h_b, _, kept_b = attention_forward(x_b, projected_b, gain_2, w_out)
        came_a, h_b = lax.optimization_barrier((came_a, h_b))
        part_a = experts_forward(0, counts_a, order, meta, all_u, weights, capacity, came_a)
        part_a, kept_near, du_rows = lax.optimization_barrier((part_a, kept_near, du_rows))
        mixed = reduce_chips(part_a)
        dh_b, g_o, g_n2, pulls_b = attention_pull(dy_b, du_rows, h_b, kept_b, gain_2, w_out)
        dx_b, g_q, g_k, g_v, g_n1 = projection_pull(x_b, dh_b, pulls_b, gain_1, w_qkv)
        dx_b, kept_near = lax.optimization_barrier((dx_b, kept_near))
        grad_w1, grad_w2, grad_w3 = experts_weights(counts_b, order, u_b, kept_near, kept_far, capacity)
        mixed, grad_w1 = lax.optimization_barrier((mixed, grad_w1))
        y_a = (h_a.astype(jnp.float32) + mixed).astype(jnp.bfloat16)
        return (y_a, dx_b, grad_w1, grad_w2, grad_w3, g_q.T.reshape((1,) + w_q.shape), g_k.T.reshape((1,) + w_k.shape), g_v.T.reshape((1,) + w_v.shape), g_o.reshape((1,) + w_o.shape), g_n1, g_n2)

    row_spec = P(('data', 'expert'), None)
    cube_spec = P(('data', 'expert'), None, None)
    quad_spec = P(('data', 'expert'), None, None, None)
    expert_spec = P('expert', None, None)
    in_specs = (row_spec, row_spec, row_spec, row_spec, row_spec, row_spec, row_spec, row_spec, row_spec, cube_spec, P(), P(), P(), P(), P(), P(), expert_spec, expert_spec, expert_spec)
    out_specs = (row_spec, row_spec, cube_spec, cube_spec, cube_spec, quad_spec, quad_spec, quad_spec, quad_spec, row_spec, row_spec)
    return jax.shard_map(local_step, mesh=mesh, in_specs=in_specs, out_specs=out_specs, check_vma=False)
```

```python
import functools

import jax
import jax.numpy as jnp
from jax import lax
from jax.experimental import pallas as pl
from jax.experimental.pallas import tpu as pltpu
from jax.sharding import PartitionSpec as P

NORM_EPS = 1e-6


def expert_map(expert_ids, slot_ids, gates, chosen):
    held = (expert_ids[None] == chosen[:, None, None]) & (slot_ids >= 0)[None]
    slot_map = jnp.max(jnp.where(held, slot_ids[None], -1), axis=2).astype(jnp.float32)
    gate_map = jnp.sum(jnp.where(held, gates.astype(jnp.float32)[None], 0.0), axis=2)
    return slot_map, gate_map


def swap(values, mask, group):
    return lax.ppermute(values, 'expert', [(i, i ^ mask) for i in range(group)])


VMEM_BYTES = 60 * 2 ** 20
NT = (((1,), (1,)), ((), ()))
TN = (((0,), (0,)), ((), ()))


def mm(lhs, rhs, dims=(((1,), (0,)), ((), ()))):
    return lax.dot_general(lhs, rhs, dims, preferred_element_type=jnp.float32)


def round_bf16(values):
    return values.astype(jnp.bfloat16).astype(jnp.float32)


def fill_sizes(capacity):
    return (capacity // 2, capacity * 9 // 16 // 16 * 16, capacity)


def by_fill(count, capacity, body):
    low = 0
    for size in fill_sizes(capacity):
        pl.when((count > low) & (count <= size))(functools.partial(body, size))
        low = size


def pair_maps(meta_ref, first):
    rows = meta_ref[0, 0]
    cols = jnp.concatenate([rows, rows], axis=0).T
    return rows[first:first + 1].astype(jnp.int32), rows[first + 1:first + 2], cols[:, first:first + 1].astype(jnp.int32), cols[:, first + 1:first + 2]


def select_rows(slot, values, size):
    rows = lax.broadcasted_iota(jnp.int32, (size, slot.shape[1]), 0)
    return jnp.where(slot == rows, values, 0.0).astype(jnp.bfloat16)


def select_cols(slot, values, size):
    cols = lax.broadcasted_iota(jnp.int32, (slot.shape[0], size), 1)
    return jnp.where(slot == cols, values, 0.0).astype(jnp.bfloat16)


def forward_kernel(capacity, bit, counts, order, meta_ref, x_ref, w1_ref, w3_ref, w2_ref, *refs):
    out_ref = refs[-1]
    place, expert = pl.program_id(0), pl.program_id(1)

    @pl.when(expert == 0)
    def _():
        out_ref[...] = refs[0][...] if len(refs) > 1 else jnp.zeros_like(out_ref)

    def body(size):
        slot_row, _, slot_col, gate_col = pair_maps(meta_ref, 0)
        buf = mm(select_rows(slot_row, 1.0, size), x_ref[0]).astype(jnp.bfloat16)
        act_1 = round_bf16(mm(buf, w1_ref[expert]))
        act_3 = round_bf16(mm(buf, w3_ref[expert]))
        hidden = (act_1 * jax.nn.sigmoid(act_1) * act_3).astype(jnp.bfloat16)
        out = mm(hidden, w2_ref[expert]).astype(jnp.bfloat16)
        out_ref[0] += mm(select_cols(slot_col, gate_col, size), out)

    by_fill(counts[order[1, 2 * place + bit], expert], capacity, body)


def backward_kernel(capacity, bit, counts, order, meta_ref, dy_ref, u_ref, w1_ref, w3_ref, w2_ref, out_ref, d_ref, hid_ref, a1_ref, a3_ref):
    place, expert = pl.program_id(0), pl.program_id(1)

    @pl.when(expert == 0)
    def _():
        out_ref[...] = jnp.zeros_like(out_ref)

    def body(size):
        slot_row, gate_row, slot_col, _ = pair_maps(meta_ref, 2)
        d_out = mm(select_rows(slot_row, gate_row, size), dy_ref[0]).astype(jnp.bfloat16)
        d_ref[0, :size, :] = d_out
        saved = u_ref[0, :size, :]
        pre_1 = round_bf16(mm(saved, w1_ref[expert]))
        pre_3 = round_bf16(mm(saved, w3_ref[expert]))
        sigma = jax.nn.sigmoid(pre_1)
        silu_1 = pre_1 * sigma
        hid_ref[0, :size, :] = (silu_1 * pre_3).astype(jnp.bfloat16)
        grad_hid = round_bf16(mm(d_out, w2_ref[expert], NT))
        grad_a1 = (grad_hid * pre_3 * sigma * (1.0 + pre_1 * (1.0 - sigma))).astype(jnp.bfloat16)
        grad_a3 = (grad_hid * silu_1).astype(jnp.bfloat16)
        a1_ref[0, :size, :] = grad_a1
        a3_ref[0, :size, :] = grad_a3
        grad_in = (mm(grad_a1, w1_ref[expert], NT) + mm(grad_a3, w3_ref[expert], NT)).astype(jnp.bfloat16)
        out_ref[0] += mm(select_cols(slot_col, 1.0, size), grad_in)

    by_fill(counts[order[1, 2 * place + bit], expert], capacity, body)


def weights_kernel(capacity, counts, order, *refs):
    expert, place = pl.program_id(0), pl.program_id(1)
    g1_ref, g2_ref, g3_ref = refs[10:]

    @pl.when(place == 0)
    def _():
        g1_ref[...] = jnp.zeros_like(g1_ref)
        g2_ref[...] = jnp.zeros_like(g2_ref)
        g3_ref[...] = jnp.zeros_like(g3_ref)

    for bit in range(2):
        u_ref, d_ref, hid_ref, a1_ref, a3_ref = refs[5 * bit:5 * bit + 5]

        def body(size):
            g2_ref[0] += mm(hid_ref[0, :size, :], d_ref[0, :size, :], TN)
            g1_ref[0] += mm(u_ref[0, :size, :], a1_ref[0, :size, :], TN)
            g3_ref[0] += mm(u_ref[0, :size, :], a3_ref[0, :size, :], TN)

        by_fill(counts[order[1, 2 * place + bit], expert], capacity, body)


def ordered_call(kernel, name, out_shape, flops, grid, in_specs, out_specs):
    return pl.pallas_call(
        kernel, out_shape=out_shape, name=name,
        grid_spec=pltpu.PrefetchScalarGridSpec(num_scalar_prefetch=2, grid=grid, in_specs=in_specs, out_specs=out_specs),
        compiler_params=pltpu.CompilerParams(dimension_semantics=('arbitrary',) * len(grid), vmem_limit_bytes=VMEM_BYTES),
        cost_estimate=pl.CostEstimate(flops=flops, bytes_accessed=2 ** 24, transcendentals=0))


def pair_specs(bit, meta, rows, weights):
    pair = pl.BlockSpec((1, 1) + meta.shape[2:], lambda i, e, counts, order: (order[1, 2 * i + bit], e, 0, 0))
    source = pl.BlockSpec((1,) + rows.shape[1:], lambda i, e, counts, order: (order[0, 2 * i + bit], 0, 0))
    whole = [pl.BlockSpec(w.shape, lambda i, e, counts, order: (0, 0, 0), pipeline_mode=pl.Buffered(1)) for w in weights]
    part = pl.BlockSpec((1,) + rows.shape[1:], lambda i, e, counts, order: (i, 0, 0))
    return pair, source, whole, part


def experts_forward(bit, counts, order, meta, rows, weights, capacity, *start):
    group, tokens, model_dim = rows.shape
    local, _, ff = weights[0].shape
    pair, source, whole, part = pair_specs(bit, meta, rows, weights)
    return ordered_call(functools.partial(forward_kernel, capacity, bit), 'experts_forward', jax.ShapeDtypeStruct((group // 2, tokens, model_dim), jnp.float32),
                        group * local * capacity * model_dim * (4 * tokens + 6 * ff) // 4, (group // 2, local), [pair, source] + whole + [part] * len(start), part)(counts, order, meta, rows, *weights, *start)


def experts_backward(bit, counts, order, meta, rows, saved, weights, capacity):
    group, tokens, model_dim = rows.shape
    local, _, ff = weights[0].shape
    pair, source, whole, part = pair_specs(bit, meta, rows, weights)
    stored = pl.BlockSpec((1, capacity, model_dim), lambda i, e, counts, order: (e, order[0, 2 * i + bit], 0))
    slots = lambda width: pl.BlockSpec((1, capacity, width), lambda i, e, counts, order: (e, i, 0))
    kept = lambda width: jax.ShapeDtypeStruct((local, group // 2 * capacity, width), jnp.bfloat16)
    return ordered_call(functools.partial(backward_kernel, capacity, bit), 'experts_backward',
                        (jax.ShapeDtypeStruct((group // 2, tokens, model_dim), jnp.float32), kept(model_dim), kept(ff), kept(ff), kept(ff)),
                        group * local * capacity * model_dim * (4 * tokens + 10 * ff) // 4, (group // 2, local),
                        [pair, source, stored] + whole, (part, slots(model_dim), slots(ff), slots(ff), slots(ff)))(counts, order, meta, rows, saved, *weights)


def experts_weights(counts, order, saved, kept_near, kept_far, capacity):
    local, slots_all, model_dim = saved.shape
    ff = kept_near[1].shape[2]
    slots = lambda width: pl.BlockSpec((1, capacity, width), lambda e, i, counts, order: (e, i, 0))
    stored = lambda bit: pl.BlockSpec((1, capacity, model_dim), lambda e, i, counts, order: (e, order[0, 2 * i + bit], 0))
    shapes = ((model_dim, ff), (ff, model_dim), (model_dim, ff))
    inner = [slots(model_dim), slots(ff), slots(ff), slots(ff)]
    return ordered_call(functools.partial(weights_kernel, capacity), 'experts_weights', tuple(jax.ShapeDtypeStruct((local,) + shape, jnp.float32) for shape in shapes),
                        local * slots_all * model_dim * 6 * ff // 2, (local, slots_all // capacity // 2),
                        [stored(0)] + inner + [stored(1)] + inner,
                        tuple(pl.BlockSpec((1,) + shape, lambda e, i, counts, order: (e, 0, 0)) for shape in shapes))(counts, order, saved, *kept_near, saved, *kept_far)


def lane_iota(shape):
    return lax.broadcasted_iota(jnp.int32, shape, len(shape) - 1)


def norm_rows(values, gain):
    scale = lax.rsqrt(jnp.mean(values * values, axis=-1, keepdims=True) + NORM_EPS)
    return values * scale, scale, (values * scale * gain).astype(jnp.bfloat16)


def norm_pull(values, gain, cotangent):
    scaled, scale, _ = norm_rows(values, gain)
    inner = cotangent * gain
    grad = scale * (inner - scaled * jnp.mean(inner * scaled, axis=-1, keepdims=True))
    return grad, jnp.sum(cotangent * scaled, axis=0, keepdims=True)


def project_kernel(score_scale, x_ref, gain_ref, w_ref, q_ref, k_ref, v_ref):
    normed = norm_rows(x_ref[...].astype(jnp.float32), gain_ref[...].astype(jnp.float32))[2]
    groups = q_ref.shape[0]
    width = q_ref.shape[2]
    mixed = round_bf16(mm(normed, w_ref[...], NT))
    for group in range(groups):
        q_ref[group] = (mixed[:, group * width:(group + 1) * width] * score_scale).astype(jnp.bfloat16)
    low = lane_iota((x_ref.shape[0], width)) < width // 2
    for start, ref in ((groups, k_ref), (groups * 3 // 2, v_ref)):
        for pair in range(groups // 2):
            both = mixed[:, (start + pair) * width:(start + pair + 1) * width]
            turned = pltpu.roll(both, width // 2, 1)
            ref[2 * pair] = jnp.where(low, both, turned).astype(jnp.bfloat16)
            ref[2 * pair + 1] = jnp.where(low, turned, both).astype(jnp.bfloat16)


def twin(rows, size):
    both = jnp.concatenate([rows, rows], axis=0)
    own = (lax.broadcasted_iota(jnp.int32, both.shape, 0) < size) == (lane_iota(both.shape) < both.shape[1] // 2)
    return jnp.where(own, both, jnp.zeros_like(both))


def untwin(columns, size):
    low = lax.broadcasted_iota(jnp.int32, (columns.shape[0], size), 0) < columns.shape[0] // 2
    return jnp.where(low, columns[:, :size], columns[:, size:]).T


def pieces(index, size):
    return ([(0, index * size)] if index else []) + [(index * size, (index + 1) * size)]


def causal_scores(k_ref, queries, start, stop, index, size):
    scores = mm(k_ref[0, start:stop, :], queries, NT)
    if start == index * size:
        column = lane_iota(scores.shape)
        row = lax.broadcasted_iota(jnp.int32, scores.shape, 0)
        scores = jnp.where(row <= jnp.where(column >= size, column - size, column), scores, -1e30)
    return scores


def attend_kernel(size, q_ref, k_ref, v_ref, out_ref, stat_ref):
    tokens = q_ref.shape[1]
    values_t = v_ref[0].T
    for index in range(tokens // size):
        rows = pl.ds(index * size, size)
        queries = twin(q_ref[0, rows, :], size)
        spans = pieces(index, size)
        scores = [causal_scores(k_ref, queries, a, b, index, size) for a, b in spans]
        top = functools.reduce(jnp.maximum, [jnp.max(part, axis=0, keepdims=True) for part in scores])
        exps = [jnp.exp(part - top) for part in scores]
        inverse = 1.0 / sum(jnp.sum(part, axis=0, keepdims=True) for part in exps)
        out = sum(mm(values_t[:, a:b], (part * inverse).astype(jnp.bfloat16)) for (a, b), part in zip(spans, exps))
        out_ref[0, rows, :] = untwin(out, size).astype(jnp.bfloat16)
        stat_ref[0, index, 0:1, :] = top
        stat_ref[0, index, 1:2, :] = inverse


def attend_pull_kernel(size, score_scale, q_ref, k_ref, v_ref, d_ref, stat_ref, dq_ref, dk_ref, dv_ref, dk_sum, dv_sum):
    tokens = q_ref.shape[1]
    width = q_ref.shape[2]
    keys_t = k_ref[0].T
    dk_sum[...] = jnp.zeros_like(dk_sum)
    dv_sum[...] = jnp.zeros_like(dv_sum)
    for index in range(tokens // size):
        rows = pl.ds(index * size, size)
        queries = twin(q_ref[0, rows, :], size)
        cotangent = twin(d_ref[0, rows, :], size)
        top = stat_ref[0, index, 0:1, :]
        inverse = stat_ref[0, index, 1:2, :]
        spans = pieces(index, size)
        probs, grads = [], []
        for a, b in spans:
            part = jnp.exp(causal_scores(k_ref, queries, a, b, index, size) - top) * inverse
            probs.append(part)
            dv_sum[a:b, :] += mm(part.astype(jnp.bfloat16), cotangent)
            grads.append(round_bf16(mm(v_ref[0, a:b, :], cotangent, NT)))
        inner = sum(jnp.sum(p * g, axis=0, keepdims=True) for p, g in zip(probs, grads))
        out = 0.0
        for (a, b), p, g in zip(spans, probs, grads):
            pull = (p * (g - inner)).astype(jnp.bfloat16)
            dk_sum[a:b, :] += mm(pull, queries)
            out = out + mm(keys_t[:, a:b], pull)
        dq_ref[0, rows, :] = (untwin(out, size) * score_scale).astype(jnp.bfloat16)
    dk_ref[0] = (dk_sum[...] + pltpu.roll(dk_sum[...], width // 2, 1)).astype(jnp.bfloat16)
    dv_ref[0] = (dv_sum[...] + pltpu.roll(dv_sum[...], width // 2, 1)).astype(jnp.bfloat16)


def merge_kernel(x_ref, gain_ref, ctx_ref, w_ref, h_ref, u_ref):
    context = jnp.concatenate([ctx_ref[group] for group in range(ctx_ref.shape[0])], axis=1)
    attn = round_bf16(mm(context, w_ref[...]))
    h_rows = (x_ref[...].astype(jnp.float32) + attn).astype(jnp.bfloat16)
    h_ref[...] = h_rows
    u_ref[...] = norm_rows(h_rows.astype(jnp.float32), gain_ref[...].astype(jnp.float32))[2]


def call(kernel, name, out_shape, flops, grid=(), **specs):
    return pl.pallas_call(
        kernel, out_shape=out_shape, grid=grid, name=name,
        compiler_params=pltpu.CompilerParams(dimension_semantics=('arbitrary',) * len(grid), vmem_limit_bytes=VMEM_BYTES),
        cost_estimate=pl.CostEstimate(flops=flops, bytes_accessed=2 ** 24, transcendentals=0), **specs)


def project(x, gain_1, w_qkv, groups):
    tokens, model_dim = x.shape
    width = model_dim // groups
    block = tokens // 4
    rows = pl.BlockSpec((block, model_dim), lambda i: (i, 0))
    head_rows = pl.BlockSpec((groups, block, width), lambda i: (0, i, 0))
    fixed = lambda array: pl.BlockSpec(array.shape, lambda i: (0, 0))
    return call(functools.partial(project_kernel, (width // 2) ** -0.5), 'project', (jax.ShapeDtypeStruct((groups, tokens, width), jnp.bfloat16),) * 3, 4 * tokens * model_dim ** 2, (4,),
                in_specs=[rows, fixed(gain_1), fixed(w_qkv)], out_specs=(head_rows,) * 3)(x, gain_1, w_qkv)


def attention_forward(x, projected, gain_2, w_out):
    query, key, value = projected
    groups, tokens, width = query.shape
    model_dim = x.shape[1]
    block = tokens // 4
    heads = jax.ShapeDtypeStruct(query.shape, jnp.bfloat16)
    like = jax.ShapeDtypeStruct(x.shape, jnp.bfloat16)
    rows = pl.BlockSpec((block, model_dim), lambda i: (i, 0))
    head_rows = pl.BlockSpec((groups, block, width), lambda i: (0, i, 0))
    fixed = lambda array: pl.BlockSpec(array.shape, lambda i: (0, 0))
    head = pl.BlockSpec((1, tokens, width), lambda g: (g, 0, 0))
    stat_shape = (groups, 4, 2, 2 * block)
    stat = pl.BlockSpec((1,) + stat_shape[1:], lambda g: (g, 0, 0, 0))
    context, stats = call(functools.partial(attend_kernel, block), 'attend', (heads, jax.ShapeDtypeStruct(stat_shape, jnp.float32)), 16 * tokens ** 2 * model_dim, (groups,),
                          in_specs=[head] * 3, out_specs=(head, stat))(query, key, value)
    h_rows, u_rows = call(merge_kernel, 'merge', (like, like), 2 * tokens * model_dim ** 2, (4,),
                          in_specs=[rows, fixed(gain_2), head_rows, fixed(w_out)], out_specs=(rows, rows))(x, gain_2, context, w_out)
    return h_rows, u_rows, (query, key, value, context, stats)


def out_pull_kernel(h_ref, dy_ref, du_ref, gain_ref, ctx_ref, w_ref, dh_ref, dctx_ref, grad_o_ref, grad_n_ref):
    groups, tokens, width = ctx_ref.shape
    gain = gain_ref[...].astype(jnp.float32)
    block = tokens // 4
    total = 0.0
    for index in range(4):
        rows = pl.ds(index * block, block)
        grad, part = norm_pull(h_ref[rows, :].astype(jnp.float32), gain, round_bf16(du_ref[rows, :]))
        total = total + part
        d_rows = (dy_ref[rows, :].astype(jnp.float32) + round_bf16(grad)).astype(jnp.bfloat16)
        dh_ref[rows, :] = d_rows
        pulled = mm(d_rows, w_ref[...], NT).astype(jnp.bfloat16)
        for group in range(groups):
            dctx_ref[group, rows, :] = pulled[:, group * width:(group + 1) * width]
    grad_n_ref[...] = round_bf16(total)
    for group in range(0, groups, 2):
        context = jnp.concatenate([ctx_ref[group], ctx_ref[group + 1]], axis=1)
        grad_o_ref[group * width:(group + 2) * width, :] = round_bf16(mm(context, dh_ref[...], TN))


def in_pull_kernel(x_ref, dh_ref, dq_ref, dk_ref, dv_ref, gain_ref, w_ref, dx_ref, gq_ref, gk_ref, gv_ref, gn_ref, normed_ref, mixed_ref):
    groups, tokens, width = dq_ref.shape
    model_dim = x_ref.shape[1]
    gain = gain_ref[...].astype(jnp.float32)
    block = tokens // 4
    low = lane_iota((block, width)) < width // 2
    total = 0.0
    for index in range(4):
        rows = pl.ds(index * block, block)
        for group in range(groups):
            mixed_ref[rows, group * width:(group + 1) * width] = dq_ref[group, rows, :]
        for start, ref in ((groups, dk_ref), (groups * 3 // 2, dv_ref)):
            for pair in range(groups // 2):
                mixed_ref[rows, (start + pair) * width:(start + pair + 1) * width] = jnp.where(low, ref[2 * pair, rows, :], ref[2 * pair + 1, rows, :])
        values = x_ref[rows, :].astype(jnp.float32)
        normed_ref[rows, :] = norm_rows(values, gain)[2]
        grad, part = norm_pull(values, gain, round_bf16(mm(mixed_ref[rows, :], w_ref[...])))
        total = total + part
        dx_ref[rows, :] = (dh_ref[rows, :].astype(jnp.float32) + round_bf16(grad)).astype(jnp.bfloat16)
    gn_ref[...] = round_bf16(total)
    half = model_dim // 2
    for start, ref in ((0, gq_ref), (2, gk_ref), (3, gv_ref)):
        for part in range(ref.shape[0] // half):
            ref[part * half:(part + 1) * half, :] = round_bf16(mm(mixed_ref[:, (start + part) * half:(start + part + 1) * half], normed_ref[...], TN))


def attention_pull(dy, du, h_rows, saved, gain_2, w_out):
    query, key, value, context, stats = saved
    groups, tokens, width = query.shape
    model_dim = dy.shape[1]
    heads = jax.ShapeDtypeStruct(query.shape, jnp.bfloat16)
    like = jax.ShapeDtypeStruct(dy.shape, jnp.bfloat16)
    wide = lambda *shape: jax.ShapeDtypeStruct(shape, jnp.float32)
    dh, d_context, grad_o, grad_n2 = call(out_pull_kernel, 'out_pull', (like, heads, wide(model_dim, model_dim), wide(1, model_dim)), 4 * tokens * model_dim ** 2)(
        h_rows, dy, du, gain_2, context, w_out)
    head = pl.BlockSpec((1, tokens, width), lambda g: (g, 0, 0))
    stat = pl.BlockSpec((1,) + stats.shape[1:], lambda g: (g, 0, 0, 0))
    d_query, d_key, d_value = call(functools.partial(attend_pull_kernel, tokens // 4, (width // 2) ** -0.5), 'attend_pull', (heads,) * 3, 40 * tokens ** 2 * model_dim, (groups,),
                                   in_specs=[head] * 4 + [stat], out_specs=(head,) * 3, scratch_shapes=[pltpu.VMEM((tokens, width), jnp.float32)] * 2)(query, key, value, d_context, stats)
    return dh, grad_o, grad_n2, (d_query, d_key, d_value)


def projection_pull(x, dh, pulls, gain_1, w_qkv):
    tokens, model_dim = x.shape
    like = jax.ShapeDtypeStruct(x.shape, jnp.bfloat16)
    wide = lambda *shape: jax.ShapeDtypeStruct(shape, jnp.float32)
    return call(
        in_pull_kernel, 'in_pull', (like, wide(model_dim, model_dim), wide(model_dim // 2, model_dim), wide(model_dim // 2, model_dim), wide(1, model_dim)), 8 * tokens * model_dim ** 2,
        scratch_shapes=[pltpu.VMEM((tokens, model_dim), jnp.bfloat16), pltpu.VMEM((tokens, 2 * model_dim), jnp.bfloat16)])(x, dh, *pulls, gain_1, w_qkv)


def solution(mesh):
    group = mesh.shape['expert']

    def local_step(x_a, x_b, dy_b, eid_a, slot_a, gate_a, eid_b, slot_b, gate_b, u_b, norm_1, norm_2, w_q, w_k, w_v, w_o, w_1, w_2, w_3):
        local_experts = w_1.shape[0]
        experts = local_experts * group
        capacity = u_b.shape[1] // group
        model_dim = x_a.shape[1]

        tokens = x_a.shape[0]
        me = lax.axis_index('expert')
        turned = me ^ jnp.arange(group, dtype=jnp.int32)
        places = (me % 2) ^ jnp.arange(group, dtype=jnp.int32)
        order = jnp.stack([places, places ^ me])
        chosen = (turned[:, None] * local_experts + jnp.arange(local_experts, dtype=jnp.int32)[None, :]).reshape(-1)
        meta = jnp.stack([*expert_map(eid_a, slot_a, gate_a, chosen), *expert_map(eid_b, slot_b, gate_b, chosen)], axis=1)
        meta = meta.reshape(group, local_experts, 4, tokens)
        meta = jnp.stack([meta[0]] + [swap(meta[r], r, group) for r in range(1, group)])
        counts_a, counts_b = (jnp.sum((meta[:, :, i] >= 0).astype(jnp.int32), axis=2) for i in (0, 2))
        weights = (w_1, w_3, w_2)

        all_dy = lax.all_gather(dy_b, 'expert', axis=0, tiled=True).reshape(group, tokens, model_dim)
        kv_heads = w_k.shape[1]
        w_qkv = jnp.concatenate([w.reshape(model_dim, -1).T for w in (w_q, w_k, w_v)], axis=0)
        w_out = w_o.reshape(-1, model_dim)
        gain_1, gain_2 = norm_1[None], norm_2[None]
        h_a, u_a, _ = attention_forward(x_a, project(x_a, gain_1, w_qkv, kv_heads), gain_2, w_out)
        all_u = lax.all_gather(u_a, 'expert', axis=0, tiled=True).reshape(group, tokens, model_dim)
        all_dy, projected_b = lax.optimization_barrier((all_dy, project(x_b, gain_1, w_qkv, kv_heads)))
        same_core = [[i for i in range(group) if i % 2 == core] for core in range(2)]
        reduce_chips = lambda part: lax.psum_scatter(part.reshape(-1, model_dim), 'expert', scatter_dimension=0, tiled=True, axis_index_groups=same_core)
        far_b, *kept_far = experts_backward(1, counts_b, order, meta, all_dy, u_b, weights, capacity)
        far_b, all_dy = lax.optimization_barrier((far_b, all_dy))
        came_b = swap(far_b, 1, group)
        near_b, *kept_near = experts_backward(0, counts_b, order, meta, all_dy, u_b, weights, capacity)
        part_b, all_u, kept_near = lax.optimization_barrier((near_b + came_b, all_u, kept_near))
        du_rows = reduce_chips(part_b)
        far_a = experts_forward(1, counts_a, order, meta, all_u, weights, capacity)
        far_a, projected_b, all_u = lax.optimization_barrier((far_a, projected_b, all_u))
        came_a = swap(far_a, 1, group)
        h_b, _, kept_b = attention_forward(x_b, projected_b, gain_2, w_out)
        came_a, h_b = lax.optimization_barrier((came_a, h_b))
        part_a = experts_forward(0, counts_a, order, meta, all_u, weights, capacity, came_a)
        part_a, kept_near, du_rows = lax.optimization_barrier((part_a, kept_near, du_rows))
        mixed = reduce_chips(part_a)
        dh_b, g_o, g_n2, pulls_b = attention_pull(dy_b, du_rows, h_b, kept_b, gain_2, w_out)
        dx_b, g_q, g_k, g_v, g_n1 = projection_pull(x_b, dh_b, pulls_b, gain_1, w_qkv)
        dx_b, kept_near = lax.optimization_barrier((dx_b, kept_near))
        grad_w1, grad_w2, grad_w3 = experts_weights(counts_b, order, u_b, kept_near, kept_far, capacity)
        mixed, grad_w1 = lax.optimization_barrier((mixed, grad_w1))
        y_a = (h_a.astype(jnp.float32) + mixed).astype(jnp.bfloat16)
        return (y_a, dx_b, grad_w1, grad_w2, grad_w3, g_q.T.reshape((1,) + w_q.shape), g_k.T.reshape((1,) + w_k.shape), g_v.T.reshape((1,) + w_v.shape), g_o.reshape((1,) + w_o.shape), g_n1, g_n2)

    row_spec = P(('data', 'expert'), None)
    cube_spec = P(('data', 'expert'), None, None)
    quad_spec = P(('data', 'expert'), None, None, None)
    expert_spec = P('expert', None, None)
    in_specs = (row_spec, row_spec, row_spec, row_spec, row_spec, row_spec, row_spec, row_spec, row_spec, cube_spec, P(), P(), P(), P(), P(), P(), expert_spec, expert_spec, expert_spec)
    out_specs = (row_spec, row_spec, cube_spec, cube_spec, cube_spec, quad_spec, quad_spec, quad_spec, quad_spec, row_spec, row_spec)
    return jax.shard_map(local_step, mesh=mesh, in_specs=in_specs, out_specs=out_specs, check_vma=False)
```
